128 devices in a mesh: grp: 8 (over x, core), dev: 16 (over y, z).
Axes of the slice: x: 4, y: 4, z: 4, core: 2. Of those that a mesh axis runs over, the one named last changes fastest.
Arguments:
- sep_inv: bfloat16 [4096, 4096], P('grp', 'dev'), may hold values from -0.125 to 0.125
- panels: bfloat16 [8, 96, 2048, 128], P('grp', 'dev'), may hold values from -1.1953125 to 1.1953125
- diag_inverse: bfloat16 [8, 96, 768, 128], P('grp', 'dev'), may hold values from -6 to 6
- widths: int32 [8, 32], P('grp'), may hold values from 1 to 6, 96 in all within a row
- ancestors: int32 [8, 32, 16], P('grp'), may hold values from 0 to 31, as said below
Outputs:
- off_diag: bfloat16 [8, 96, 2048, 128], P('grp', 'dev')
- diag_panels: bfloat16 [8, 96, 768, 128], P('grp', 'dev')
The draws below stay inside these ranges and needn't reach their ends.
Inputs may be any that keep to these rules, and one draw needn't show every extreme that they name: `widths`: each row of a subtree sums to 96. `ancestors`: each supernode's list holds 16 different separator tile numbers in increasing order.
All inputs are finite; a program needn't handle non-finite values.
Results may differ from the reference program's by a relative error of at most 0.0046.
Values may be sent and summed in bfloat16 or wider, within the bound.
No kernel may reach another device: no remote copies, remote signals or barrier semaphores. Data moves between devices by JAX's collectives and lax.ppermute only.
A program may use at most 320 MiB of HBM per device.

```python
import math
import jax
import jax.numpy as jnp
import numpy as np
from jax import lax

SEP = 4096
B = 128
ANC = 16
MAXU = 6
GROUPS = 8
UNITS = 96
NSG = 32
WMAX = 768


def draw_ancestors(key, part):
    count_blocks = SEP // B
    noise = jax.random.randint(key, (GROUPS, NSG, count_blocks), 0, 4 * count_blocks)
    index = jnp.arange(count_blocks, dtype=jnp.int32)
    scores = (noise + index) * count_blocks + index
    chosen = lax.top_k(scores, ANC)[1]
    return jnp.sort(chosen, axis=-1).astype(jnp.int32)


def block_levels(rng, shape, shards, low, high):
    def one(dim, parts):
        heights = jax.random.uniform(jax.random.fold_in(jax.random.fold_in(rng, 6), dim), (parts,), jnp.float32, low / len(shards), high / len(shards))
        return jnp.repeat(jnp.exp(heights), shape[dim] // parts).reshape((-1,) + (1,) * (len(shape) - dim - 1))

    loudness = one(*shards[0])
    for cut in shards[1:]:
        loudness = loudness * one(*cut)
    return loudness


def profile(count, total, reach, skew):
    weights = [(1 << 20) // math.isqrt(standing ** skew) + 1 for standing in range(2, count + 1)]
    spare, counts = total - reach - (count - 1), [1] * (count - 1)
    while spare > 0:
        candidates = [i for i in range(count - 1) if counts[i] < reach]
        whole, left = sum([weights[i] for i in candidates]), spare
        for i in candidates:
            more = min(reach - counts[i], max(1, left * weights[i] // whole), spare)
            counts[i] = counts[i] + more
            spare = spare - more
    return np.array([reach] + counts)


def uneven_parts(stream_key, count, total, limit, lean):
    if count == 2:
        one = jax.random.randint(stream_key, (), max(1, total - limit), min(limit, total - 1) + 1)
        return jnp.stack([one, total - one])
    sizes = jnp.asarray(profile(count, total, limit, lean), jnp.int32)
    couples = (count - 1) // 2
    giver, receiver = sizes[1:1 + 2 * couples:2], sizes[2:2 + 2 * couples:2]
    room = jnp.minimum(giver - 1, limit - receiver)
    passed = jax.random.randint(jax.random.fold_in(stream_key, 1), (couples,), 0, 1 << 20) % (room + 1)
    sizes = sizes.at[1:1 + 2 * couples:2].set(giver - passed).at[2:2 + 2 * couples:2].set(receiver + passed)
    return sizes[jax.random.permutation(jax.random.fold_in(stream_key, 2), count)]


def scatter_about(stream_key, dims, deviation, most, split=(), held_as=jnp.bfloat16):
    array = jax.random.normal(stream_key, dims, jnp.float32) * deviation
    if len(split) > 0:
        array = block_levels(stream_key, dims, split, -0.22, 0.18) * array
    return jnp.clip(array, min=-most, max=most).astype(held_as)


def setup_inputs(seed: int = 0) -> dict:
    seeds = jax.random.split(jax.random.key(seed), 6)
    return {
        "sep_inv": scatter_about(seeds[0], (SEP, SEP), (ANC * B) ** -0.5, 0.125, ((0, 8), (1, 16))),
        "panels": scatter_about(seeds[1], (GROUPS, UNITS, ANC * B, B), 0.2, 1.1953125, ((0, 8), (1, 16))),
        "diag_inverse": scatter_about(seeds[2], (GROUPS, UNITS, WMAX, B), 1.0, 6.0, ((0, 8), (1, 16))),
        "widths": jax.vmap(lambda own: uneven_parts(own, NSG, UNITS, MAXU, 1))(jax.random.split(seeds[3], GROUPS)).reshape((GROUPS, NSG)).astype(jnp.int32),
        "ancestors": draw_ancestors(jax.random.fold_in(seeds[5], 71), 0),
    }


def reference(sep_inv, panels, diag_inverse, widths, ancestors):
    units = panels.shape[1]
    count_blocks = SEP // B
    tiles = sep_inv.astype(jnp.float32).reshape(count_blocks, B, count_blocks, B).transpose(0, 2, 1, 3)

    def per_group(group_args):
        panel_g, dinv_g, width_g, anc_g = group_args
        ends = jnp.cumsum(width_g).astype(jnp.int32)
        starts = ends - width_g
        position = jnp.arange(units, dtype=jnp.int32)
        owner = jnp.sum((ends[None, :] <= position[:, None]).astype(jnp.int32), axis=1).astype(jnp.int32)
        column = position - starts[owner]
        width_u = width_g[owner]
        blocks = anc_g[owner]
        padded = jnp.pad(panel_g, ((MAXU - 1, MAXU - 1), (0, 0), (0, 0)))

        def per_unit(unit_idx):
            chosen = blocks[unit_idx]
            picked = tiles[chosen[:, None], chosen[None, :]]
            panel_u = panel_g[unit_idx].astype(jnp.float32).reshape(ANC, B, B)
            product = jnp.einsum('abij,bjc->aic', picked, panel_u).reshape(ANC * B, B)
            result_x = (-product).astype(jnp.bfloat16)
            start_at = (unit_idx + MAXU - 1 - column[unit_idx]).astype(jnp.int32)
            related = lax.dynamic_slice_in_dim(padded, start_at, MAXU, 0)
            inner = jnp.einsum('jrb,rc->jbc', related.astype(jnp.float32), result_x.astype(jnp.float32))
            keep = (jnp.arange(MAXU, dtype=jnp.int32) < width_u[unit_idx]).astype(jnp.float32)
            diag_block = (dinv_g[unit_idx].astype(jnp.float32).reshape(MAXU, B, B) - inner) * keep[:, None, None]
            return result_x, diag_block.reshape(MAXU * B, B).astype(jnp.bfloat16)

        return lax.map(per_unit, jnp.arange(units, dtype=jnp.int32))

    off_diag, diag_panels = lax.map(per_group, (panels, diag_inverse, widths, ancestors))
    return off_diag, diag_panels
```

```python
import functools

import jax
import jax.numpy as jnp
from jax import lax
from jax.experimental import pallas as pl
from jax.experimental.pallas import tpu as pltpu
from jax.sharding import Mesh, PartitionSpec as P

T = 128
ALL = ("x", "core", "y", "z")


def compute(meta, row_at, col_at, parts, panels, turned, dinv):
    units, rows, _ = panels.shape
    anc = rows // T
    wmax = dinv.shape[1] // T
    side = wmax - 1
    per_part = [p.shape[0] for p in parts]
    n_parts = len(parts)
    tiles = sum(per_part)
    group = 4

    def kernel(*refs):
        meta_ref, row_ref, col_ref = refs[:3]
        part_refs = refs[3 : 3 + n_parts]
        pan_ref, left_ref, own_ref, right_ref, dinv_ref, off_ref, diag_ref = refs[3 + n_parts : 10 + n_parts]
        sep_v, turn_v, rhs_v, res_v, sem, tsem = refs[10 + n_parts :]
        base = 0
        copies = []
        for i, p in enumerate(part_refs):
            copies.append(pltpu.make_async_copy(p, sep_v.at[pl.ds(base, per_part[i])], sem.at[i]))
            base += per_part[i]
        for c in copies:
            c.start()
        turns = [
            pltpu.make_async_copy(left_ref, turn_v.at[pl.ds(0, side)], tsem.at[0]),
            pltpu.make_async_copy(own_ref, turn_v.at[pl.ds(side, units)], tsem.at[1]),
            pltpu.make_async_copy(right_ref, turn_v.at[pl.ds(side + units, side)], tsem.at[2]),
        ]
        for c in turns:
            c.start()
        for c in copies + turns:
            c.wait()

        def job(t, carry):
            @pl.when(meta_ref[t, 0] == 1)
            def _():
                mate = meta_ref[t, 1]
                first = meta_ref[t, 2]
                width = meta_ref[t, 3]
                rhs_v[:, :T] = pan_ref[t]
                rhs_v[:, T:] = pan_ref[mate]

                def rows_of(a0, carry):
                    lhs = []
                    for i in range(group):
                        r = meta_ref[t, 4 + a0 * group + i]
                        kind = row_ref[1, r]
                        at = row_ref[0, r]
                        lhs.append(
                            jnp.concatenate(
                                [sep_v[at + col_ref[kind, meta_ref[t, 4 + b]]] for b in range(anc)], axis=1
                            )
                        )
                    lhs = jnp.concatenate(lhs, axis=0)
                    prod = jnp.dot(lhs, rhs_v[...], preferred_element_type=jnp.float32)
                    got = (-prod).astype(jnp.bfloat16)
                    here = pl.ds(pl.multiple_of(a0 * group * T, T), group * T)
                    res_v[here, :] = got
                    off_ref[t, here, :] = got[:, :T]
                    off_ref[mate, here, :] = got[:, T:]
                    return carry

                lax.fori_loop(0, anc // group, rows_of, 0)
                for j in range(wmax):
                    inner = jnp.dot(turn_v[first + j], res_v[...], preferred_element_type=jnp.float32)
                    live = j < width
                    here = slice(j * T, (j + 1) * T)
                    for k, u in ((1, mate), (0, t)):
                        new = dinv_ref[u, here, :].astype(jnp.float32) - inner[:, k * T : (k + 1) * T]
                        diag_ref[u, here, :] = jnp.where(live, new, 0.0).astype(jnp.bfloat16)

            return carry

        lax.fori_loop(0, units, job, 0)

    any_spec = pl.BlockSpec(memory_space=pl.ANY)
    vmem_spec = pl.BlockSpec(memory_space=pltpu.VMEM)
    smem_spec = pl.BlockSpec(memory_space=pltpu.SMEM)
    return pl.pallas_call(
        kernel,
        out_shape=(
            jax.ShapeDtypeStruct(panels.shape, jnp.bfloat16),
            jax.ShapeDtypeStruct(dinv.shape, jnp.bfloat16),
        ),
        in_specs=[smem_spec] * 3 + [any_spec] * n_parts + [vmem_spec] + [any_spec] * 3 + [vmem_spec],
        out_specs=(vmem_spec, vmem_spec),
        scratch_shapes=[
            pltpu.VMEM((tiles, T, T), jnp.bfloat16),
            pltpu.VMEM((units + 2 * side, T, rows), jnp.bfloat16),
            pltpu.VMEM((rows, 2 * T), jnp.bfloat16),
            pltpu.VMEM((rows, 2 * T), jnp.bfloat16),
            pltpu.SemaphoreType.DMA((n_parts,)),
            pltpu.SemaphoreType.DMA((3,)),
        ],
        compiler_params=pltpu.CompilerParams(vmem_limit_bytes=64 * 1024 * 1024),
        cost_estimate=pl.CostEstimate(flops=2 * 7 * rows * rows * T * units // 6, bytes_accessed=50_000_000, transcendentals=0),
        name="units",
    )(meta, row_at, col_at, *parts, panels, *turned, dinv)


def unit_table(widths, ancestors, place, units):
    wmax = 6
    ends = jnp.cumsum(widths)
    starts = ends - widths
    local = jnp.arange(units, dtype=jnp.int32)
    position = place * units + local
    owner = jnp.sum((ends[None, :] <= position[:, None]).astype(jnp.int32), axis=1)
    hot = (jnp.arange(widths.shape[0], dtype=jnp.int32)[None, :] == owner[:, None]).astype(jnp.int32)
    column = position - jnp.sum(hot * starts[None, :], axis=1)
    width = jnp.sum(hot * widths[None, :], axis=1)
    blocks = jnp.sum(hot[:, :, None] * ancestors[None, :, :], axis=1)
    run = jnp.minimum(column, local)
    leads = (run % 2 == 0).astype(jnp.int32)
    mate = jnp.where((column + 1 < width) & (local + 1 < units), local + 1, local)
    first = (wmax - 1) + local - column
    return jnp.concatenate([jnp.stack([leads, mate, first, width], axis=1), blocks], axis=1).astype(jnp.int32)


def on_device(sep, panels, dinv, widths, ancestors):
    panels, dinv, widths, ancestors = panels[0], dinv[0], widths[0], ancestors[0]
    units = panels.shape[0]
    side = dinv.shape[1] // T - 1
    n_y, n_z = lax.axis_size("y"), lax.axis_size("z")
    n_dev = n_y * n_z
    rt, ct = sep.shape[0] // T, sep.shape[1] // T
    shard = sep.reshape(rt, T, ct, T).transpose(0, 2, 1, 3)
    whole = lax.all_gather(shard[None], ALL, axis=0, tiled=True)
    n_tiles = whole.shape[0] * rt * ct
    whole = whole.reshape(n_tiles, T, T)
    steps = [(i, i + 1) for i in range(n_dev - 1)]
    left = lax.ppermute(panels[units - side :], ("y", "z"), steps)
    right = lax.ppermute(panels[:side], ("y", "z"), [(b, a) for a, b in steps])
    turned = [v.transpose(0, 2, 1) for v in (left, panels, right)]
    place = lax.axis_index("y") * n_z + lax.axis_index("z")
    meta = unit_table(widths, ancestors, place, units)
    count = lax.axis_size("x") * lax.axis_size("core") * rt
    tile = jnp.arange(count, dtype=jnp.int32)
    row_at = jnp.stack([(tile // rt) * (n_dev * rt * ct) + (tile % rt) * ct, jnp.zeros_like(tile)])
    col_at = ((tile // ct) * (rt * ct) + tile % ct)[None]
    off, diag = compute(meta, row_at, col_at, [whole], panels, turned, dinv)
    return off[None], diag[None]


def solution(mesh):
    grid = Mesh(mesh.devices.reshape(4, 2, 4, 4), ALL)
    grp, dev = ("x", "core"), ("y", "z")
    placed = (P(grp, dev), P(grp, dev), P(grp, dev), P(grp), P(grp))
    return jax.shard_map(
        on_device, mesh=grid, in_specs=placed, out_specs=(P(grp, dev), P(grp, dev)), check_vma=False
    )
```

```python
import math

import jax
import jax.numpy as jnp
import numpy as np
from jax import lax
from jax.experimental import pallas as pl
from jax.experimental.pallas import tpu as pltpu
from jax.sharding import Mesh, PartitionSpec as P


T = 128
ALL = ("x", "core", "y", "z")


def compute(meta, row_at, col_at, parts, panels, turned, dinv):
    units, rows, _ = panels.shape
    anc = rows // T
    wmax = dinv.shape[1] // T
    side = wmax - 1
    per_part = [p.shape[0] for p in parts]
    n_parts = len(parts)
    tiles = sum(per_part)
    group = 4

    def kernel(*refs):
        meta_ref, row_ref, col_ref = refs[:3]
        part_refs = refs[3 : 3 + n_parts]
        pan_ref, left_ref, own_ref, right_ref, dinv_ref, off_ref, diag_ref = refs[3 + n_parts : 10 + n_parts]
        sep_v, turn_v, rhs_v, res_v, sem, tsem = refs[10 + n_parts :]
        base = 0
        copies = []
        for i, p in enumerate(part_refs):
            copies.append(pltpu.make_async_copy(p, sep_v.at[pl.ds(base, per_part[i])], sem.at[i]))
            base += per_part[i]
        for c in copies:
            c.start()
        turns = [
            pltpu.make_async_copy(left_ref, turn_v.at[pl.ds(0, side)], tsem.at[0]),
            pltpu.make_async_copy(own_ref, turn_v.at[pl.ds(side, units)], tsem.at[1]),
            pltpu.make_async_copy(right_ref, turn_v.at[pl.ds(side + units, side)], tsem.at[2]),
        ]
        for c in turns:
            c.start()
        for c in copies + turns:
            c.wait()

        def job(t, carry):
            @pl.when(meta_ref[t, 0] == 1)
            def _():
                mate = meta_ref[t, 1]
                first = meta_ref[t, 2]
                width = meta_ref[t, 3]
                rhs_v[:, :T] = pan_ref[t]
                rhs_v[:, T:] = pan_ref[mate]

                def rows_of(a0, carry):
                    lhs = []
                    for i in range(group):
                        r = meta_ref[t, 4 + a0 * group + i]
                        kind = row_ref[1, r]
                        at = row_ref[0, r]
                        lhs.append(
                            jnp.concatenate(
                                [sep_v[at + col_ref[kind, meta_ref[t, 4 + b]]] for b in range(anc)], axis=1
                            )
                        )
                    lhs = jnp.concatenate(lhs, axis=0)
                    prod = jnp.dot(lhs, rhs_v[...], preferred_element_type=jnp.float32)
                    got = (-prod).astype(jnp.bfloat16)
                    here = pl.ds(pl.multiple_of(a0 * group * T, T), group * T)
                    res_v[here, :] = got
                    off_ref[t, here, :] = got[:, :T]
                    off_ref[mate, here, :] = got[:, T:]
                    return carry

                lax.fori_loop(0, anc // group, rows_of, 0)
                for j in range(wmax):
                    inner = jnp.dot(turn_v[first + j], res_v[...], preferred_element_type=jnp.float32)
                    live = j < width
                    here = slice(j * T, (j + 1) * T)
                    for k, u in ((1, mate), (0, t)):
                        new = dinv_ref[u, here, :].astype(jnp.float32) - inner[:, k * T : (k + 1) * T]
                        diag_ref[u, here, :] = jnp.where(live, new, 0.0).astype(jnp.bfloat16)

            return carry

        lax.fori_loop(0, units, job, 0)

    any_spec = pl.BlockSpec(memory_space=pl.ANY)
    vmem_spec = pl.BlockSpec(memory_space=pltpu.VMEM)
    smem_spec = pl.BlockSpec(memory_space=pltpu.SMEM)
    return pl.pallas_call(
        kernel,
        out_shape=(
            jax.ShapeDtypeStruct(panels.shape, jnp.bfloat16),
            jax.ShapeDtypeStruct(dinv.shape, jnp.bfloat16),
        ),
        in_specs=[smem_spec] * 3 + [any_spec] * n_parts + [vmem_spec] + [any_spec] * 3 + [vmem_spec],
        out_specs=(vmem_spec, vmem_spec),
        scratch_shapes=[
            pltpu.VMEM((tiles, T, T), jnp.bfloat16),
            pltpu.VMEM((units + 2 * side, T, rows), jnp.bfloat16),
            pltpu.VMEM((rows, 2 * T), jnp.bfloat16),
            pltpu.VMEM((rows, 2 * T), jnp.bfloat16),
            pltpu.SemaphoreType.DMA((n_parts,)),
            pltpu.SemaphoreType.DMA((3,)),
        ],
        compiler_params=pltpu.CompilerParams(vmem_limit_bytes=64 * 1024 * 1024),
        cost_estimate=pl.CostEstimate(flops=2 * 7 * rows * rows * T * units // 6, bytes_accessed=50_000_000, transcendentals=0),
        name="units",
    )(meta, row_at, col_at, *parts, panels, *turned, dinv)


def unit_table(widths, ancestors, place, units):
    wmax = 6
    ends = jnp.cumsum(widths)
    starts = ends - widths
    local = jnp.arange(units, dtype=jnp.int32)
    position = place * units + local
    owner = jnp.sum((ends[None, :] <= position[:, None]).astype(jnp.int32), axis=1)
    hot = (jnp.arange(widths.shape[0], dtype=jnp.int32)[None, :] == owner[:, None]).astype(jnp.int32)
    column = position - jnp.sum(hot * starts[None, :], axis=1)
    width = jnp.sum(hot * widths[None, :], axis=1)
    blocks = jnp.sum(hot[:, :, None] * ancestors[None, :, :], axis=1)
    run = jnp.minimum(column, local)
    leads = (run % 2 == 0).astype(jnp.int32)
    mate = jnp.where((column + 1 < width) & (local + 1 < units), local + 1, local)
    first = (wmax - 1) + local - column
    return jnp.concatenate([jnp.stack([leads, mate, first, width], axis=1), blocks], axis=1).astype(jnp.int32)


ROUTES = ((("z", "y", "x"), ("y", "z", "x")), (("x", "z", "y"), ("z", "x", "y")))
AXIS = {"x": 0, "y": 2, "z": 3}


def neighbours(sizes, dims, by):
    out = []
    total = math.prod(sizes)
    for i in range(total):
        at = list(np.unravel_index(i, sizes))
        k = AXIS[dims[at[1]]]
        at[k] = (at[k] + by) % sizes[k]
        out.append((i, int(np.ravel_multi_index(at, sizes))))
    return out


def gathered(shard):
    sizes = [lax.axis_size(a) for a in ALL]
    halves = len(ROUTES[0])
    rt = shard.shape[0]

    def send(v, dims, by):
        return lax.ppermute(v, ALL, neighbours(sizes, dims, by))

    def swap(v):
        return lax.ppermute(v, "core", [(0, 1), (1, 0)])

    parts = []
    for h in range(halves):
        block = shard[h * rt // halves : (h + 1) * rt // halves][None]
        legs = [tuple(ROUTES[c][h][leg] for c in range(2)) for leg in range(3)]
        for dims in legs[:2]:
            up, down, across = (send(block, dims, by) for by in (1, -1, 2))
            block = jnp.concatenate([block, down, across, up], axis=0)
        up, down = (send(block, legs[2], by) for by in (1, -1))
        across = send(up if h == 0 else down, legs[2], 1 if h == 0 else -1)
        parts += [block, down, across, up]
    parts += [swap(v) for v in parts]
    return [v.reshape(-1, T, T) for v in parts]


def tile_tables(rt, ct):
    sizes = {a: lax.axis_size(a) for a in ALL}
    ring, halves = sizes["x"], len(ROUTES[0])
    inner = rt // halves * ct
    r = jnp.arange(ring * 2 * rt, dtype=jnp.int32)
    c = jnp.arange(sizes["y"] * sizes["z"] * ct, dtype=jnp.int32)
    ahead = lambda axis, v: (v - lax.axis_index(axis) + ring) % ring
    off_x = ahead("x", r // (2 * rt))
    off = {"y": ahead("y", c // (sizes["z"] * ct)), "z": ahead("z", c // ct % sizes["z"])}
    core, half = r // rt % 2, r % rt // (rt // halves)
    kind = core * halves + half
    weight = {a: [] for a in "xyz"}
    for route in (ROUTES[k // halves][k % halves] for k in range(2 * halves)):
        for leg, axis in enumerate(route):
            weight[axis].append(inner * ring**leg)
    part = inner * ring**3
    row = jnp.where(core == lax.axis_index("core"), 0, halves * part) + half * part + r % (rt // halves) * ct
    for k in range(2 * halves):
        row = row + jnp.where(kind == k, weight["x"][k], 0) * off_x
    col = jnp.stack([weight["y"][k] * off["y"] + weight["z"][k] * off["z"] + c % ct for k in range(2 * halves)])
    return jnp.stack([row, kind]), col


def on_device(sep, panels, dinv, widths, ancestors):
    panels, dinv, widths, ancestors = panels[0], dinv[0], widths[0], ancestors[0]
    units = panels.shape[0]
    side = dinv.shape[1] // T - 1
    n_y, n_z = lax.axis_size("y"), lax.axis_size("z")
    n_dev = n_y * n_z
    rt, ct = sep.shape[0] // T, sep.shape[1] // T
    shard = sep.reshape(rt, T, ct, T).transpose(0, 2, 1, 3)
    parts = gathered(shard)
    steps = [(i, i + 1) for i in range(n_dev - 1)]
    left = lax.ppermute(panels[units - side :], ("y", "z"), steps)
    right = lax.ppermute(panels[:side], ("y", "z"), [(b, a) for a, b in steps])
    turned = [v.transpose(0, 2, 1) for v in (left, panels, right)]
    place = lax.axis_index("y") * n_z + lax.axis_index("z")
    meta = unit_table(widths, ancestors, place, units)
    row_at, col_at = tile_tables(rt, ct)
    off, diag = compute(meta, row_at, col_at, parts, panels, turned, dinv)
    return off[None], diag[None]


def solution(mesh):
    grid = Mesh(mesh.devices.reshape(4, 2, 4, 4), ALL)
    grp, dev = ("x", "core"), ("y", "z")
    placed = (P(grp, dev), P(grp, dev), P(grp, dev), P(grp), P(grp))

    return jax.shard_map(on_device, mesh=grid, in_specs=placed, out_specs=(P(grp, dev), P(grp, dev)), check_vma=False)
```
